32 devices in a mesh: grp: 2 (over x), seq: 16 (over z, y, core).
Axes of the slice: x: 2, y: 2, z: 4, core: 2. Of those that a mesh axis runs over, the one named last changes fastest.
Arguments:
- cont_query: bfloat16 [64, 32, 2560], P(('grp', 'seq')), parts along dimension 0, may hold values from -180 to 180
- cont_key: bfloat16 [64, 32, 512], P(('grp', 'seq')), parts along dimension 0, may hold values from -6 to 6
- cont_value: bfloat16 [64, 32, 512], P(('grp', 'seq')), parts along dimension 0, may hold values from -6 to 6
- prefix_key: bfloat16 [4, 2048, 512], P('grp', 'seq'), parts along dimension 0, may hold values from -7 to 7
- prefix_value: bfloat16 [4, 2048, 512], P('grp', 'seq'), parts along dimension 0, may hold values from -6 to 6
- out_weight: bfloat16 [2560, 2560], P(None, 'seq'), may hold values from -0.125 to 0.125
- norm_gain: float32 [2560], replicated, may hold values from 0.5 to 1.5
- lm_head: bfloat16 [2560, 76032], P(None, 'seq'), may hold values from -18 to 18
- target_ids: int32 [64, 32], P(('grp', 'seq')), parts along dimension 0, may hold values from 0 to 76031
- cont_len: int32 [64], P(('grp', 'seq')), parts along dimension 0, may hold values from 8 to 32
- prompt_len: int32 [4], P('grp'), parts along dimension 0, may hold values from 1024 to 2048
- group_of: int32 [64], P('grp'), parts along dimension 0, may hold values from 0 to 1, as said below
- rewards: float32 [64], P(('grp', 'seq')), parts along dimension 0, may hold values from -13 to 13
Outputs:
- token_logprob: float32 [64, 32], P(('grp', 'seq')), parts along dimension 0
- advantage: float32 [64], P(('grp', 'seq')), parts along dimension 0
- objective: float32 [64], P(('grp', 'seq')), parts along dimension 0
The draws below stay inside these ranges and needn't reach their ends.
There are 2 independent parts, one for each index of `grp`. The reference program is written for one: setup_inputs(seed, part) draws one part's arguments, and reference() takes and returns one part's arrays. A program takes and returns all parts, laid end to end along the dimension named above; an argument that names none is the same for every part. Nothing has to cross between parts.
Inputs may be any that keep to these rules, and one draw needn't show every extreme that they name: `group_of`: each of the 2 prompts is named by exactly 16 continuations.
All inputs are finite; a program needn't handle non-finite values.
Results may differ from the reference program's by a relative error of at most 0.0026.
Values may be sent and summed in bfloat16 or wider, within the bound.
No kernel may reach another device: no remote copies, remote signals or barrier semaphores. Data moves between devices by JAX's collectives and lax.ppermute only.
A program may use at most 128 MiB of HBM per device.

```python
import math
import jax
import jax.numpy as jnp
import numpy as np
from jax import lax

D = 2560
QH = 20
KVH = 4
HD = 128
VOCAB = 76032
GROUP = 16
CLEN = 32
PROMPT = 2048
CONTS = 32
PROMPTS = 2
N_SEQ = 16


def draw_groups(key):
    shuffled = jax.random.permutation(jax.random.fold_in(key, 11), CONTS)
    return (shuffled // GROUP).astype(jnp.int32)


def draw_group_of(key, part):
    return draw_groups(key)


def draw_prefix_key(key, part):
    drawn = jnp.clip(jax.random.normal(jax.random.fold_in(key, 13), (PROMPTS, PROMPT, KVH * HD), jnp.float32), -6.0, 6.0)
    return drawn.astype(jnp.bfloat16)


def draw_cont_query(key, part):
    drawn = jnp.clip(jax.random.normal(jax.random.fold_in(key, 14), (CONTS, CLEN, QH * HD), jnp.float32), -6.0, 6.0)
    return drawn.astype(jnp.bfloat16)


def draw_lm_head(key, part):
    drawn = jnp.clip(jax.random.normal(jax.random.fold_in(key, 19), (D, VOCAB), jnp.float32), -6.0, 6.0)
    column_scale = jnp.full((1, VOCAB), 3.0 / math.sqrt(D), jnp.float32)
    return (drawn * column_scale).astype(jnp.bfloat16)


def draw_rewards(key, part):
    groups = draw_groups(key)
    spread = jnp.exp(jax.random.uniform(jax.random.fold_in(key, 16), (PROMPTS,), jnp.float32, math.log(0.05), math.log(2.0)))
    offset = jax.random.uniform(jax.random.fold_in(key, 17), (PROMPTS,), jnp.float32, -1.0, 1.0)
    jitter = jnp.clip(jax.random.normal(jax.random.fold_in(key, 18), (CONTS,), jnp.float32), -6.0, 6.0)
    return offset[groups] + spread[groups] * jitter


def place_ends(array, own_key, smallest, largest):
    shape = array.shape
    index_at = [jax.random.randint(jax.random.fold_in(own_key, axis), (), 0, shape[axis]) for axis in range(len(shape))]
    array = array.at[tuple(index_at)].set(smallest)
    longest = shape.index(max(shape))
    index_at[longest] = (index_at[longest] + 1) % shape[longest]
    return array.at[tuple(index_at)].set(largest)


def level_of(stream_key, dims, pieces, least, largest):
    factor_of = 1.0
    for axis_at, blocks in pieces:
        draws = jax.random.uniform(jax.random.fold_in(jax.random.fold_in(stream_key, 6), axis_at), (blocks,), jnp.float32, least / len(pieces), largest / len(pieces))
        factor_of = factor_of * jnp.repeat(jnp.exp(draws), dims[axis_at] // blocks).reshape((-1,) + (1,) * (len(dims) - 1 - axis_at))
    return factor_of


def skewed_wide(stream_key, dims, number_of, lean):
    loads = [min(1 << octave, number_of + 1 - (1 << octave)) * (1 << 20) // math.isqrt((1 << octave) ** lean) + 1 for octave in range((number_of + 1).bit_length()) if 1 << octave <= number_of]
    width = 1 + sum(loads) // (1 << 30)
    listing = np.cumsum(np.array([max(1, weight // width) for weight in loads]))
    ticket = jax.random.randint(jax.random.fold_in(stream_key, 1), dims, 0, int(listing[len(loads) - 1]))
    start = jnp.left_shift(1, jnp.searchsorted(jnp.asarray(listing, jnp.int32), ticket, side="right").astype(jnp.int32))
    grade = start - 1 + jax.random.randint(jax.random.fold_in(stream_key, 4), dims, 0, 1 << 30) % jnp.minimum(start, number_of + 1 - start)
    return jax.random.permutation(jax.random.fold_in(stream_key, 2), number_of)[grade].astype(jnp.int32)


def bell_draw(own_key, shape, scale, bound, shards=(), held_as=jnp.bfloat16):
    values = scale * jax.random.normal(own_key, shape, jnp.float32)
    if shards:
        values = values * level_of(own_key, shape, shards, -0.22, 0.18)
    return jnp.clip(values, -bound, bound).astype(held_as)


def setup_inputs(seed: int = 0, part: int = 0) -> dict:
    key_list = jax.random.split(jax.random.key(seed), 14)
    part_keys = jax.random.split(jax.random.fold_in(key_list[13], part), 14)
    return {
        "cont_query": draw_cont_query(jax.random.fold_in(jax.random.fold_in(key_list[13], part), 71), part),
        "cont_key": bell_draw(part_keys[1], (CONTS, CLEN, KVH * HD), 1.0, 6.0, ((0, 16),)),
        "cont_value": bell_draw(part_keys[2], (CONTS, CLEN, KVH * HD), 1.0, 6.0, ((0, 16),)),
        "prefix_key": draw_prefix_key(jax.random.fold_in(jax.random.fold_in(key_list[13], part), 71), part),
        "prefix_value": bell_draw(part_keys[4], (PROMPTS, PROMPT, KVH * HD), 1.0, 6.0, ((1, 16),)),
        "out_weight": bell_draw(key_list[5], (QH * HD, D), (QH * HD) ** -0.5, 0.125, ((1, 16),)),
        "norm_gain": jnp.clip(1.0 + 0.1 * jax.random.normal(key_list[6], (D,), jnp.float32), 0.5, 1.5),
        "lm_head": draw_lm_head(jax.random.fold_in(key_list[13], 71), part),
        "target_ids": place_ends(skewed_wide(part_keys[8], (CONTS, CLEN), VOCAB, 2), jax.random.fold_in(part_keys[8], 3), 0, VOCAB - 1).astype(jnp.int32),
        "cont_len": place_ends(jax.random.randint(part_keys[9], (CONTS,), CLEN // 4, CLEN + 1), jax.random.fold_in(part_keys[9], 1), CLEN // 4, CLEN).astype(jnp.int32),
        "prompt_len": jax.random.randint(part_keys[10], (PROMPTS,), PROMPT // 2, PROMPT + 1).astype(jnp.int32),
        "group_of": draw_group_of(jax.random.fold_in(jax.random.fold_in(key_list[13], part), 71), part),
        "rewards": draw_rewards(jax.random.fold_in(jax.random.fold_in(key_list[13], part), 71), part),
    }


NEGATIVE = -1e+30
EPSILON = 1e-06
REWARD_FLOOR = 0.25

def normalize(hidden, norm_gain):
    widened = hidden.astype(jnp.float32)
    factor = lax.rsqrt(lax.optimization_barrier(jnp.mean(widened * widened, axis=-1, keepdims=True)) + EPSILON)
    return (widened * factor * norm_gain).astype(jnp.bfloat16)

def shard_stats(normed, token_ids, head, vocab_offset):
    logits = jnp.dot(normed, head, preferred_element_type=jnp.float32)
    maximum = lax.optimization_barrier(jnp.max(logits, axis=1))
    total_mass = lax.optimization_barrier(jnp.sum(jnp.exp(logits - maximum[:, None]), axis=1))
    columns = vocab_offset + jnp.arange(head.shape[1], dtype=jnp.int32)
    picked = lax.optimization_barrier(jnp.sum(jnp.where(token_ids[:, None] == columns[None, :], logits, 0.0), axis=1))
    return (maximum, total_mass, picked)

def join_stats(first, second):
    maximum = jnp.maximum(first[0], second[0])
    total_mass = first[1] * jnp.exp(first[0] - maximum) + second[1] * jnp.exp(second[0] - maximum)
    return (maximum, total_mass, first[2] + second[2])

def reference(cont_query, cont_key, cont_value, prefix_key, prefix_value, out_weight, norm_gain, lm_head, target_ids, cont_len, prompt_len, group_of, rewards):
    per_group = QH // KVH
    position = jnp.arange(CLEN, dtype=jnp.int32)
    causal = position[None, :] <= position[:, None]
    highest = lax.Precision.HIGHEST

    def attend(index):
        prompt = group_of[index]
        key_rows = jnp.concatenate([prefix_key[prompt], cont_key[index]], axis=0).astype(jnp.float32).reshape(PROMPT + CLEN, KVH, HD)
        value_rows = jnp.concatenate([prefix_value[prompt], cont_value[index]], axis=0).astype(jnp.float32).reshape(PROMPT + CLEN, KVH, HD)
        queries = cont_query[index].astype(jnp.float32).reshape(CLEN, KVH, per_group, HD)
        scores = jnp.einsum('tkgd,skd->tkgs', queries, key_rows, precision=highest) * HD ** (-0.5)
        early = jnp.broadcast_to((jnp.arange(PROMPT, dtype=jnp.int32) < prompt_len[prompt])[None, :], (CLEN, PROMPT))
        visible = jnp.concatenate([early, causal], axis=1)[:, None, None, :]
        scores = jnp.where(visible, scores, NEGATIVE)
        maximum = lax.optimization_barrier(jnp.max(scores, axis=-1, keepdims=True))
        weights = jnp.where(visible, jnp.exp(scores - maximum), 0.0)
        total = lax.optimization_barrier(jnp.sum(weights, axis=-1))
        mixed = jnp.einsum('tkgs,skd->tkgd', weights, value_rows, precision=highest) / total[..., None]
        return mixed.astype(jnp.bfloat16).reshape(CLEN, QH * HD)
    attended = lax.map(attend, jnp.arange(CONTS, dtype=jnp.int32)).reshape(CONTS * CLEN, QH * HD)
    hidden = jnp.dot(attended, out_weight, preferred_element_type=jnp.float32).astype(jnp.bfloat16)
    normed = normalize(hidden, norm_gain)
    token_ids = target_ids.reshape(CONTS * CLEN)
    block = VOCAB // N_SEQ

    def vocab_step(step, running):
        head = lax.dynamic_slice_in_dim(lm_head, step * block, block, 1)
        stats = shard_stats(normed, token_ids, head, step * block)
        return join_stats(running, stats)
    start_stats = (jnp.full((CONTS * CLEN,), NEGATIVE, jnp.float32), jnp.zeros((CONTS * CLEN,), jnp.float32), jnp.zeros((CONTS * CLEN,), jnp.float32))
    maximum, total_mass, picked = lax.fori_loop(0, N_SEQ, vocab_step, start_stats)
    logprob = (picked - maximum - jnp.log(total_mass)).reshape(CONTS, CLEN)
    live = position[None, :] < cont_len[:, None]
    token_logprob = jnp.where(live, logprob, 0.0)
    same_group = (group_of[:, None] == group_of[None, :]).astype(jnp.float32)
    group_mean = jnp.dot(same_group, rewards, precision=highest) / GROUP
    deviation = rewards[None, :] - group_mean[:, None]
    spread = jnp.sqrt(lax.optimization_barrier(jnp.sum(same_group * deviation * deviation, axis=1)) / (GROUP - 1))
    advantage = (rewards - group_mean) / jnp.maximum(spread, REWARD_FLOOR)
    objective = advantage * lax.optimization_barrier(jnp.sum(token_logprob, axis=1)) / cont_len.astype(jnp.float32)
    return (token_logprob, advantage, objective)
```

```python
import math

import jax
import jax.numpy as jnp
from jax import lax
from jax.experimental import pallas as pl
from jax.experimental.pallas import tpu as pltpu
from jax.sharding import PartitionSpec as P

HD = 128
GROUP = 16
PLANE = 4
TILE = 512


NEGATIVE = -1e30
EPSILON = 1e-06
REWARD_FLOOR = 0.25


def swap(x, mask, devices):
    return lax.ppermute(x, "seq", [(i, i ^ mask) for i in range(devices)])


def spread_masks(devices, heads):
    masks = [PLANE * heads * (1 << b) for b in range((devices // (PLANE * heads)).bit_length() - 1)]
    return masks + [2, 1]


def gather_all(x, devices, heads):
    pieces = {0: x}
    for k in range(1, heads):
        pieces[PLANE * k] = swap(x, PLANE * k, devices)
    return widen(pieces, devices, heads)


def widen(pieces, devices, heads):
    for mask in spread_masks(devices, heads):
        for m in list(pieces):
            pieces[m ^ mask] = swap(pieces[m], mask, devices)
    return [pieces[m] for m in range(devices)]


def attention_kernel(group, lens, own_ref, pos_ref, *refs, per_group, span):
    pieces, out_ref = refs[:-1], refs[-1]
    at = pl.program_id(0)
    prompt = group[at]
    rows = per_group * span
    queries = own_ref[0, :rows]
    own_key = own_ref[0, rows:rows + span]
    own_value = own_ref[0, rows + span:]
    keys = jnp.concatenate([ref[0, prompt] for ref in pieces], axis=0)
    values = jnp.concatenate([ref[1, prompt] for ref in pieces], axis=0)
    contract = (((1,), (1,)), ((), ()))
    far = lax.dot_general(queries, keys, contract, preferred_element_type=jnp.float32) * HD ** (-0.5)
    near = lax.dot_general(queries, own_key, contract, preferred_element_type=jnp.float32) * HD ** (-0.5)
    far = jnp.where(pos_ref[...] < lens[at], far, NEGATIVE)
    row = lax.broadcasted_iota(jnp.int32, near.shape, 0) % span
    near = jnp.where(lax.broadcasted_iota(jnp.int32, near.shape, 1) <= row, near, NEGATIVE)
    peak = jnp.maximum(jnp.max(far, axis=1, keepdims=True), jnp.max(near, axis=1, keepdims=True))
    far = jnp.exp(far - peak)
    near = jnp.exp(near - peak)
    total = jnp.sum(far, axis=1, keepdims=True) + jnp.sum(near, axis=1, keepdims=True)
    mixed = jnp.dot(far.astype(jnp.bfloat16), values, preferred_element_type=jnp.float32)
    mixed += jnp.dot(near.astype(jnp.bfloat16), own_value, preferred_element_type=jnp.float32)
    mixed = (mixed / total).astype(jnp.bfloat16)
    for j in range(per_group):
        out_ref[0, :, j * HD:(j + 1) * HD] = mixed[j * span:(j + 1) * span]


def project_kernel(index, weight_ref, *refs, heads, fold):
    pieces, out_ref, hold = refs[:-2], refs[-2], refs[-1]
    own = index[0]
    head = (own // PLANE) % heads
    rows = pieces[0].shape[1]
    weight = jnp.concatenate([weight_ref[head ^ k] for k in range(heads)], axis=0)
    for m in range(len(pieces)):
        if (m // PLANE) % heads:
            continue
        left = jnp.concatenate(
            [
                jnp.concatenate([pieces[m + PLANE * k][k ^ t] for k in range(heads)], axis=1)
                for t in range(heads)
            ],
            axis=0,
        )
        product = jnp.dot(left, weight, preferred_element_type=jnp.float32)
        for t in range(heads):
            hold[own ^ (m + PLANE * t)] = product[t * rows:(t + 1) * rows]
    cols = hold.shape[2]
    part = len(pieces) // fold
    for a in range(fold):
        block = hold[a * part:(a + 1) * part].reshape(part * rows, cols)
        out_ref[:, a * cols:(a + 1) * cols] = block.astype(jnp.bfloat16)


def score_kernel(index, ids_ref, gain_ref, hidden_ref, head_ref, out_ref, normed, top, mass, pick, *, fold, vocab):
    step = pl.program_id(0)
    own = index[0]
    devices = hidden_ref.shape[0]
    part = hidden_ref.shape[1]
    cols = hidden_ref.shape[2] // fold

    @pl.when(step == 0)
    def _():
        for a in range(fold):
            wide = jnp.concatenate(
                [
                    hidden_ref[d ^ own, :, a * cols:(a + 1) * cols].astype(jnp.float32)
                    for d in range(devices)
                ],
                axis=1,
            )
            factor = lax.rsqrt(jnp.mean(wide * wide, axis=1, keepdims=True) + EPSILON)
            normed[a * part:(a + 1) * part] = (wide * factor * gain_ref[...]).astype(jnp.bfloat16)
        top[...] = jnp.full_like(top, NEGATIVE)
        mass[...] = jnp.zeros_like(mass)
        pick[...] = jnp.zeros_like(pick)

    logits = jnp.dot(normed[...], head_ref[...], preferred_element_type=jnp.float32)
    lane = lax.broadcasted_iota(jnp.int32, (1, HD), 1) + step * TILE
    wanted = ids_ref[...] - own * vocab
    wanted = jnp.where(wanted < vocab, wanted, -1)
    groups = []
    peak = top[...]
    found = pick[...]
    for j in range(TILE // HD):
        column = lane + j * HD
        piece = jnp.where(column < vocab, logits[:, j * HD:(j + 1) * HD], NEGATIVE)
        found += jnp.where(wanted == column, piece, 0.0)
        peak = jnp.maximum(peak, piece)
        groups.append(piece)
    total = mass[...] * jnp.exp(top[...] - peak)
    for piece in groups:
        total += jnp.exp(piece - peak)
    top[...] = peak
    mass[...] = total
    pick[...] = found

    @pl.when(step == pl.num_programs(0) - 1)
    def _():
        best = jnp.max(peak, axis=1, keepdims=True)
        whole = jnp.sum(total * jnp.exp(peak - best), axis=1, keepdims=True)
        chosen = jnp.sum(found, axis=1, keepdims=True)
        at = lax.broadcasted_iota(jnp.int32, out_ref.shape, 1)
        out_ref[...] = jnp.where(at == 0, best, jnp.where(at == 1, whole, chosen))


def per_device(
    cont_query,
    cont_key,
    cont_value,
    prefix_key,
    prefix_value,
    out_weight,
    norm_gain,
    lm_head,
    target_ids,
    cont_len,
    prompt_len,
    group_of,
    rewards,
):
    devices = lax.axis_size("seq")
    conts, span, query_width = cont_query.shape
    own_rows = conts * span
    kv_width = cont_key.shape[2]
    heads = kv_width // HD
    per_group = query_width // kv_width
    prompts, piece_len, _ = prefix_key.shape
    index = lax.axis_index("seq").astype(jnp.int32)
    head = (index // PLANE) % heads
    own_groups = lax.dynamic_slice_in_dim(group_of, index * conts, conts)

    def by_head(x):
        return x.reshape(x.shape[:2] + (heads, HD)).transpose(2, 0, 1, 3)

    prefix = jnp.stack([by_head(prefix_key), by_head(prefix_value)], axis=1)
    queries = cont_query.reshape(conts, span, heads, per_group, HD).transpose(2, 0, 3, 1, 4)
    own = jnp.concatenate(
        [queries.reshape(heads, conts, per_group * span, HD), by_head(cont_key), by_head(cont_value)],
        axis=2,
    )
    at_head = lambda x, k: lax.dynamic_index_in_dim(x, head ^ k, 0, False)
    far = {0: at_head(prefix, 0)}
    for k in range(1, heads):
        far[PLANE * k] = swap(at_head(prefix, k), PLANE * k, devices)
    near = [at_head(own, 0)]
    near += [swap(at_head(own, k), PLANE * k, devices) for k in range(1, heads)]
    near = jnp.concatenate(near, axis=0)
    far = widen(far, devices, heads)
    shared = lax.all_gather(
        jnp.concatenate([target_ids.reshape(own_rows).astype(jnp.float32), rewards]), "seq", axis=0
    )
    every_id = shared[:, :own_rows].astype(jnp.int32).reshape(devices * own_rows, 1)
    every_reward = shared[:, own_rows:].reshape(devices * conts)
    order = index ^ jnp.arange(devices, dtype=jnp.int32)
    position = order[:, None] * piece_len + jnp.arange(piece_len, dtype=jnp.int32)[None, :]
    holders = index ^ (PLANE * jnp.arange(heads, dtype=jnp.int32))
    near_groups = group_of.reshape(devices, conts)[holders].reshape(heads * conts)
    near_lens = prompt_len[near_groups]
    grown = pltpu.CompilerParams(vmem_limit_bytes=60 * 1024 * 1024)
    still = lambda shape: pl.BlockSpec(shape, lambda *_: (0,) * len(shape))
    width = per_group * HD
    attended = pl.pallas_call(
        lambda *refs: attention_kernel(*refs, per_group=per_group, span=span),
        grid_spec=pltpu.PrefetchScalarGridSpec(
            num_scalar_prefetch=2,
            grid=(heads * conts,),
            in_specs=[
                pl.BlockSpec((1,) + near.shape[1:], lambda i, *_: (i, 0, 0)),
                still((1, devices * piece_len)),
            ]
            + [still(far[0].shape)] * devices,
            out_specs=pl.BlockSpec((1, span, width), lambda i, *_: (i, 0, 0)),
        ),
        out_shape=jax.ShapeDtypeStruct((heads * conts, span, width), jnp.bfloat16),
        compiler_params=grown,
    )(near_groups, near_lens, near, position.reshape(1, -1), *far)
    pieces = gather_all(attended.reshape(heads, own_rows, width), devices, heads)
    cols = out_weight.shape[1]
    fold = HD // math.gcd(cols, HD)
    tokens = devices * own_rows
    hidden_cols = pl.pallas_call(
        lambda *refs: project_kernel(*refs, heads=heads, fold=fold),
        grid_spec=pltpu.PrefetchScalarGridSpec(
            num_scalar_prefetch=1,
            grid=(1,),
            in_specs=[still((heads, width, cols))] + [still(pieces[0].shape)] * devices,
            out_specs=still((tokens // fold, fold * cols)),
            scratch_shapes=[pltpu.VMEM((devices, own_rows, cols), jnp.float32)],
        ),
        out_shape=jax.ShapeDtypeStruct((tokens // fold, fold * cols), jnp.bfloat16),
        compiler_params=grown,
    )(index[None], out_weight.reshape(heads, width, cols), *pieces)
    hidden = jnp.stack(gather_all(hidden_cols, devices, heads))
    vocab = lm_head.shape[1]
    features = lm_head.shape[0]
    stats = pl.pallas_call(
        lambda *refs: score_kernel(*refs, fold=fold, vocab=vocab),
        grid_spec=pltpu.PrefetchScalarGridSpec(
            num_scalar_prefetch=1,
            grid=(pl.cdiv(vocab, TILE),),
            in_specs=[
                still((tokens, 1)),
                still((1, features)),
                pl.BlockSpec(hidden.shape, lambda *_: (0, 0, 0), pipeline_mode=pl.Buffered(1)),
                pl.BlockSpec((features, TILE), lambda i, *_: (0, i)),
            ],
            out_specs=still((tokens, HD)),
            scratch_shapes=[pltpu.VMEM((tokens, features), jnp.bfloat16)]
            + [pltpu.VMEM((tokens, HD), jnp.float32)] * 3,
        ),
        out_shape=jax.ShapeDtypeStruct((tokens, HD), jnp.float32),
        compiler_params=grown,
    )(index[None], every_id, norm_gain.reshape(1, features), hidden, lm_head)
    shares = stats[:, :3].T.reshape(3, devices, own_rows).transpose(1, 0, 2)
    shares = lax.all_to_all(shares, "seq", split_axis=0, concat_axis=0, tiled=True)
    maximum = jnp.max(shares[:, 0], axis=0)
    total_mass = jnp.sum(shares[:, 1] * jnp.exp(shares[:, 0] - maximum[None, :]), axis=0)
    picked = jnp.sum(shares[:, 2], axis=0)
    logprob = (picked - maximum - jnp.log(total_mass)).reshape(conts, span)
    live = jnp.arange(span, dtype=jnp.int32)[None, :] < cont_len[:, None]
    token_logprob = jnp.where(live, logprob, 0.0)
    own_rows_groups = (own_groups[:, None] == group_of[None, :]).astype(jnp.float32)
    group_mean = jnp.dot(own_rows_groups, every_reward, precision=lax.Precision.HIGHEST) / GROUP
    deviation = every_reward[None, :] - group_mean[:, None]
    spread = jnp.sqrt(jnp.sum(own_rows_groups * deviation * deviation, axis=1) / (GROUP - 1))
    advantage = (rewards - group_mean) / jnp.maximum(spread, REWARD_FLOOR)
    objective = advantage * jnp.sum(token_logprob, axis=1) / cont_len.astype(jnp.float32)
    return (token_logprob, advantage, objective)


def solution(mesh):
    placed = (
        P(("grp", "seq"), None, None),
        P(("grp", "seq"), None, None),
        P(("grp", "seq"), None, None),
        P("grp", "seq", None),
        P("grp", "seq", None),
        P(None, "seq"),
        P(),
        P(None, "seq"),
        P(("grp", "seq"), None),
        P(("grp", "seq")),
        P("grp"),
        P("grp"),
        P(("grp", "seq")),
    )
    return jax.shard_map(
        per_device,
        mesh=mesh,
        in_specs=placed,
        out_specs=(P(("grp", "seq"), None), P(("grp", "seq")), P(("grp", "seq"))),
        check_vma=False,
    )
```

```python
import math

import jax
import jax.numpy as jnp
from jax import lax
from jax.experimental import pallas as pl
from jax.experimental.pallas import tpu as pltpu
from jax.sharding import PartitionSpec as P

HD = 128
GROUP = 16
PLANE = 4
STEPS = 3
HALVES = 2


NEGATIVE = -1e30
EPSILON = 1e-06
REWARD_FLOOR = 0.25


def swap(x, mask, devices):
    return lax.ppermute(x, "seq", [(i, i ^ mask) for i in range(devices)])


def spread_masks(devices, heads):
    masks = [PLANE * heads * (1 << b) for b in range((devices // (PLANE * heads)).bit_length() - 1)]
    return masks + [2, 1]


def gather_all(x, devices, heads):
    pieces = {0: x}
    for k in range(1, heads):
        pieces[PLANE * k] = swap(x, PLANE * k, devices)
    return widen(pieces, devices, heads)


def widen(pieces, devices, heads):
    for mask in spread_masks(devices, heads):
        for m in list(pieces):
            pieces[m ^ mask] = swap(pieces[m], mask, devices)
    return [pieces[m] for m in range(devices)]


def attention_kernel(group, lens, own_ref, pos_ref, *refs, per_group, span):
    pieces, out_ref = refs[:-1], refs[-1]
    at = pl.program_id(0)
    prompt = group[at]
    rows = per_group * span
    queries = own_ref[0, :rows]
    own_key = own_ref[0, rows:rows + span]
    own_value = own_ref[0, rows + span:]
    keys = jnp.concatenate([ref[0, prompt] for ref in pieces], axis=0)
    values = jnp.concatenate([ref[1, prompt] for ref in pieces], axis=0)
    contract = (((1,), (1,)), ((), ()))
    far = lax.dot_general(queries, keys, contract, preferred_element_type=jnp.float32) * HD ** (-0.5)
    near = lax.dot_general(queries, own_key, contract, preferred_element_type=jnp.float32) * HD ** (-0.5)
    far = jnp.where(pos_ref[...] < lens[at], far, NEGATIVE)
    row = lax.broadcasted_iota(jnp.int32, near.shape, 0) % span
    near = jnp.where(lax.broadcasted_iota(jnp.int32, near.shape, 1) <= row, near, NEGATIVE)
    peak = jnp.maximum(jnp.max(far, axis=1, keepdims=True), jnp.max(near, axis=1, keepdims=True))
    far = jnp.exp(far - peak)
    near = jnp.exp(near - peak)
    total = jnp.sum(far, axis=1, keepdims=True) + jnp.sum(near, axis=1, keepdims=True)
    mixed = jnp.dot(far.astype(jnp.bfloat16), values, preferred_element_type=jnp.float32)
    mixed += jnp.dot(near.astype(jnp.bfloat16), own_value, preferred_element_type=jnp.float32)
    mixed = (mixed / total).astype(jnp.bfloat16)
    for j in range(per_group):
        out_ref[0, :, j * HD:(j + 1) * HD] = mixed[j * span:(j + 1) * span]


def project_kernel(index, weight_ref, *refs, heads, fold):
    pieces, outs, hold = refs[:-1 - HALVES], refs[-1 - HALVES:-1], refs[-1]
    own = index[0]
    head = (own // PLANE) % heads
    rows = pieces[0].shape[1]
    width = weight_ref.shape[1] // heads
    weight = jnp.concatenate(
        [weight_ref[:, pl.ds(pl.multiple_of((head ^ k) * width, HD), width)] for k in range(heads)],
        axis=1,
    )
    for m in range(len(pieces)):
        if (m // PLANE) % heads:
            continue
        left = jnp.concatenate(
            [
                jnp.concatenate([pieces[m + PLANE * k][k ^ t] for k in range(heads)], axis=1)
                for t in range(heads)
            ],
            axis=0,
        )
        product = lax.dot_general(
            left, weight, (((1,), (1,)), ((), ())), preferred_element_type=jnp.float32
        )
        for t in range(heads):
            hold[own ^ (m + PLANE * t)] = product[t * rows:(t + 1) * rows]
    cols = hold.shape[2]
    part = len(pieces) // fold
    for a in range(fold):
        block = hold[a * part:(a + 1) * part].reshape(part * rows, cols)
        height = part * rows // HALVES
        for i, out_ref in enumerate(outs):
            out_ref[:, a * cols:(a + 1) * cols] = block[i * height:(i + 1) * height].astype(jnp.bfloat16)


def score_kernel(index, ids_ref, gain_ref, head_ref, *refs, fold, vocab):
    pieces, (out_ref, hold, normed, top, mass, pick) = refs[:-6], refs[-6:]
    step = pl.program_id(0)
    own = index[0]
    part = pieces[0].shape[0]
    cols = pieces[0].shape[1] // fold
    tile = head_ref.shape[0]

    @pl.when(step == 0)
    def _():
        for m, ref in enumerate(pieces):
            hold[m] = ref[...]
        for a in range(fold):
            wide = jnp.concatenate(
                [
                    hold[d ^ own, :, a * cols:(a + 1) * cols].astype(jnp.float32)
                    for d in range(len(pieces))
                ],
                axis=1,
            )
            factor = lax.rsqrt(jnp.mean(wide * wide, axis=1, keepdims=True) + EPSILON)
            normed[a * part:(a + 1) * part] = (wide * factor * gain_ref[...]).astype(jnp.bfloat16)
        top[...] = jnp.full_like(top, NEGATIVE)
        mass[...] = jnp.zeros_like(mass)
        pick[...] = jnp.zeros_like(pick)

    logits = lax.dot_general(
        head_ref[...], normed[...], (((1,), (1,)), ((), ())), preferred_element_type=jnp.float32
    )
    entry = lax.broadcasted_iota(jnp.int32, logits.shape, 0)
    if vocab % tile:
        logits = jnp.where(entry < vocab - step * tile, logits, NEGATIVE)
    wanted = ids_ref[...] - own * vocab
    wanted = jnp.where(wanted < vocab, wanted, -1) - step * tile
    peak = jnp.maximum(top[...], jnp.max(logits, axis=0, keepdims=True))
    mass[...] = mass[...] * jnp.exp(top[...] - peak) + jnp.sum(
        jnp.exp(logits - peak), axis=0, keepdims=True
    )
    pick[...] += jnp.sum(jnp.where(entry == wanted, logits, 0.0), axis=0, keepdims=True)
    top[...] = peak

    @pl.when(step == pl.num_programs(0) - 1)
    def _():
        out_ref[0:1] = top[...]
        out_ref[1:2] = mass[...]
        out_ref[2:3] = pick[...]


def per_device(
    cont_query,
    cont_key,
    cont_value,
    prefix_key,
    prefix_value,
    out_weight,
    norm_gain,
    lm_head,
    target_ids,
    cont_len,
    prompt_len,
    group_of,
    rewards,
):
    devices = lax.axis_size("seq")
    conts, span, query_width = cont_query.shape
    own_rows = conts * span
    kv_width = cont_key.shape[2]
    heads = kv_width // HD
    per_group = query_width // kv_width
    prompts, piece_len, _ = prefix_key.shape
    index = lax.axis_index("seq").astype(jnp.int32)
    head = (index // PLANE) % heads
    own_groups = lax.dynamic_slice_in_dim(group_of, index * conts, conts)

    def by_head(x):
        return x.reshape(x.shape[:2] + (heads, HD)).transpose(2, 0, 1, 3)

    prefix = jnp.stack([by_head(prefix_key), by_head(prefix_value)], axis=1)
    queries = cont_query.reshape(conts, span, heads, per_group, HD).transpose(2, 0, 3, 1, 4)
    own = jnp.concatenate(
        [queries.reshape(heads, conts, per_group * span, HD), by_head(cont_key), by_head(cont_value)],
        axis=2,
    )
    at_head = lambda x, k: lax.dynamic_index_in_dim(x, head ^ k, 0, False)
    far = {0: at_head(prefix, 0)}
    for k in range(1, heads):
        far[PLANE * k] = swap(at_head(prefix, k), PLANE * k, devices)
    near = [at_head(own, 0)]
    near += [swap(at_head(own, k), PLANE * k, devices) for k in range(1, heads)]
    near = jnp.concatenate(near, axis=0)
    far = widen(far, devices, heads)
    shared = jnp.concatenate([target_ids.reshape(own_rows).astype(jnp.float32), rewards])[None]
    for bit in range(devices.bit_length() - 1):
        shared = jnp.concatenate([shared, swap(shared, 1 << bit, devices)])
    order = index ^ jnp.arange(devices, dtype=jnp.int32)
    shared = shared[order]
    every_id = shared[:, :own_rows].astype(jnp.int32)
    every_reward = shared[:, own_rows:].reshape(devices * conts)
    position = order[:, None] * piece_len + jnp.arange(piece_len, dtype=jnp.int32)[None, :]
    holders = index ^ (PLANE * jnp.arange(heads, dtype=jnp.int32))
    near_groups = group_of.reshape(devices, conts)[holders].reshape(heads * conts)
    near_lens = prompt_len[near_groups]
    grown = pltpu.CompilerParams(vmem_limit_bytes=60 * 1024 * 1024)
    still = lambda shape: pl.BlockSpec(shape, lambda *_: (0,) * len(shape))
    width = per_group * HD
    attended = pl.pallas_call(
        lambda *refs: attention_kernel(*refs, per_group=per_group, span=span),
        grid_spec=pltpu.PrefetchScalarGridSpec(
            num_scalar_prefetch=2,
            grid=(heads * conts,),
            in_specs=[
                pl.BlockSpec((1,) + near.shape[1:], lambda i, *_: (i, 0, 0)),
                still((1, devices * piece_len)),
            ]
            + [still(far[0].shape)] * devices,
            out_specs=pl.BlockSpec((1, span, width), lambda i, *_: (i, 0, 0)),
        ),
        out_shape=jax.ShapeDtypeStruct((heads * conts, span, width), jnp.bfloat16),
        compiler_params=grown,
    )(near_groups, near_lens, near, position.reshape(1, -1), *far)
    pieces = gather_all(attended.reshape(heads, own_rows, width), devices, heads)
    cols = out_weight.shape[1]
    fold = HD // math.gcd(cols, HD)
    tokens = devices * own_rows
    height = tokens // (fold * HALVES)
    vocab = lm_head.shape[1]
    features = lm_head.shape[0]
    hidden_cols = pl.pallas_call(
        lambda *refs: project_kernel(*refs, heads=heads, fold=fold),
        grid_spec=pltpu.PrefetchScalarGridSpec(
            num_scalar_prefetch=1,
            grid=(1,),
            in_specs=[still((cols, features))] + [still(pieces[0].shape)] * devices,
            out_specs=[still((height, fold * cols))] * HALVES,
            scratch_shapes=[pltpu.VMEM((devices, own_rows, cols), jnp.float32)],
        ),
        out_shape=[jax.ShapeDtypeStruct((height, fold * cols), jnp.bfloat16)] * HALVES,
        compiler_params=grown,
    )(index[None], out_weight.T, *pieces)
    ids = every_id.reshape(fold, HALVES, height).transpose(1, 0, 2).reshape(HALVES, 1, fold * height)
    tile = -(-vocab // (STEPS * 16)) * 16
    once = lambda shape: pl.BlockSpec(
        shape, lambda *_: (0,) * len(shape), pipeline_mode=pl.Buffered(1)
    )
    stats = []
    for half in range(HALVES):
        hidden = gather_all(hidden_cols[half], devices, heads)
        stats.append(
            pl.pallas_call(
                lambda *refs: score_kernel(*refs, fold=fold, vocab=vocab),
                grid_spec=pltpu.PrefetchScalarGridSpec(
                    num_scalar_prefetch=1,
                    grid=(pl.cdiv(vocab, tile),),
                    in_specs=[
                        still((1, fold * height)),
                        still((1, features)),
                        pl.BlockSpec((tile, features), lambda i, *_: (i, 0)),
                    ]
                    + [once((height, fold * cols))] * devices,
                    out_specs=still((8, fold * height)),
                    scratch_shapes=[
                        pltpu.VMEM((devices, height, fold * cols), jnp.bfloat16),
                        pltpu.VMEM((fold * height, features), jnp.bfloat16),
                    ]
                    + [pltpu.VMEM((1, fold * height), jnp.float32)] * 3,
                ),
                out_shape=jax.ShapeDtypeStruct((8, fold * height), jnp.float32),
                compiler_params=grown,
            )(index[None], ids[half], norm_gain.reshape(1, features), lm_head.T, *hidden)
        )
    shares = jnp.stack([part[:3].reshape(3, fold, height) for part in stats], axis=2)
    shares = shares.reshape(3, devices, own_rows).transpose(1, 0, 2)
    shares = lax.all_to_all(shares, "seq", split_axis=0, concat_axis=0, tiled=True)
    maximum = jnp.max(shares[:, 0], axis=0)
    total_mass = jnp.sum(shares[:, 1] * jnp.exp(shares[:, 0] - maximum[None, :]), axis=0)
    picked = jnp.sum(shares[:, 2], axis=0)
    logprob = (picked - maximum - jnp.log(total_mass)).reshape(conts, span)
    live = jnp.arange(span, dtype=jnp.int32)[None, :] < cont_len[:, None]
    token_logprob = jnp.where(live, logprob, 0.0)
    own_rows_groups = (own_groups[:, None] == group_of[None, :]).astype(jnp.float32)
    group_mean = jnp.dot(own_rows_groups, every_reward, precision=lax.Precision.HIGHEST) / GROUP
    deviation = every_reward[None, :] - group_mean[:, None]
    spread = jnp.sqrt(jnp.sum(own_rows_groups * deviation * deviation, axis=1) / (GROUP - 1))
    advantage = (rewards - group_mean) / jnp.maximum(spread, REWARD_FLOOR)
    objective = advantage * jnp.sum(token_logprob, axis=1) / cont_len.astype(jnp.float32)
    return (token_logprob, advantage, objective)


def solution(mesh):
    placed = (
        P(("grp", "seq"), None, None),
        P(("grp", "seq"), None, None),
        P(("grp", "seq"), None, None),
        P("grp", "seq", None),
        P("grp", "seq", None),
        P(None, "seq"),
        P(),
        P(None, "seq"),
        P(("grp", "seq"), None),
        P(("grp", "seq")),
        P("grp"),
        P("grp"),
        P(("grp", "seq")),
    )
    return jax.shard_map(
        per_device,
        mesh=mesh,
        in_specs=placed,
        out_specs=(P(("grp", "seq"), None), P(("grp", "seq")), P(("grp", "seq"))),
        check_vma=False,
    )
```
